256 devices in a mesh: row: 32 (over z_hi, x, y), col: 8 (over z_lo, core).
Axes of the slice: x: 4, y: 4, z: 8 (z_hi: 2, z_lo: 4; z = z_hi * 4 + z_lo), core: 2. Of those that a mesh axis runs over, the one named last changes fastest.
Arguments:
- query_proj: bfloat16 [768, 768, 128], P('row', 'col'), may hold values from -8 to 8
- key_proj: bfloat16 [768, 768, 128], P('row', 'col'), may hold values from -8 to 8
- value_proj: bfloat16 [768, 768, 128], P('row', 'col'), may hold values from -6 to 6
- pair_bias: bfloat16 [4, 768, 768], P(None, 'col', 'row'), may hold values from -9 to 9
- pair_mask: int32 [768, 768], P('row', 'col'), may hold values 0 or 1
- grad_out: bfloat16 [768, 768, 128], P('row', 'col'), may hold values from -18 to 18
Outputs:
- grad_query: bfloat16 [768, 768, 128], P('row', 'col')
- grad_key: bfloat16 [768, 768, 128], P('row', 'col')
- grad_value: bfloat16 [768, 768, 128], P('row', 'col')
- grad_bias: float32 [4, 768, 768], P(None, 'col', 'row')
The draws below stay inside these ranges and needn't reach their ends.
All inputs are finite; a program needn't handle non-finite values. No bound on the sum of `pair_mask` on one device may be relied on, other than what follows from the above.
Results may differ from the reference program's by a relative error of at most 0.0096.
Values may be sent and summed in bfloat16 or wider, within the bound.
No kernel may reach another device: no remote copies, remote signals or barrier semaphores. Data moves between devices by JAX's collectives and lax.ppermute only.
A program may use at most 128 MiB of HBM per device.

```python
import math
import jax
import jax.numpy as jnp
from jax import lax

HEADS = 4
HEAD_DIM = 32
RESIDUES = 768
CHANNELS = 128


def field_draw(key):
    return jnp.clip(jax.random.normal(key, (RESIDUES, RESIDUES, CHANNELS), jnp.float32), -6.0, 6.0)


def draw_query_proj(key, part):
    values_drawn = field_draw(jax.random.fold_in(key, 1))
    return values_drawn.astype(jnp.bfloat16)


def draw_key_proj(key, part):
    values_drawn = field_draw(jax.random.fold_in(key, 2))
    return values_drawn.astype(jnp.bfloat16)


def place_ends(values, own_key, least, top_value):
    dims = values.shape
    index_at = [jax.random.randint(jax.random.fold_in(own_key, axis), (), 0, dims[axis]) for axis in range(len(dims))]
    values = values.at[tuple(index_at)].set(least)
    longest = dims.index(max(dims))
    index_at[longest] = (index_at[longest] + 1) % dims[longest]
    return values.at[tuple(index_at)].set(top_value)


def steps_of(own_key, extent, split, least, largest):
    loudness, own = 1.0, jax.random.fold_in(own_key, 6)
    for dim, shards_of in split:
        heights = jnp.exp(jax.random.uniform(jax.random.fold_in(own, dim), (shards_of,), jnp.float32, least / len(split), largest / len(split)))
        loudness = loudness * jnp.repeat(heights, extent[dim] // shards_of).reshape([-1 if axis == dim else 1 for axis in range(len(extent))])
    return loudness


def noise(key, shape, deviation, limit, cuts=(), held_as=jnp.bfloat16):
    level = steps_of(key, shape, cuts, -0.22, 0.18) if cuts else 1.0
    result = jax.random.normal(key, shape, jnp.float32) * deviation * level
    return jnp.minimum(jnp.maximum(result, -limit), limit).astype(held_as)


def setup_inputs(seed: int = 0) -> dict:
    seeds = jax.random.split(jax.random.key(seed), 7)
    query_proj = draw_query_proj(jax.random.fold_in(seeds[6], 71), 0)
    key_proj = draw_key_proj(jax.random.fold_in(seeds[6], 71), 0)
    value_proj = noise(seeds[2], (RESIDUES, RESIDUES, CHANNELS), 1.0, 6.0, ((0, 32), (1, 8)))
    pair_bias = noise(seeds[3], (HEADS, RESIDUES, RESIDUES), 1.5, 9.0, ((1, 8), (2, 32)))
    pair_mask = place_ends((jax.random.randint(seeds[4], (RESIDUES, RESIDUES), 0, 4) < 3).astype(jnp.int32), jax.random.fold_in(seeds[4], 1), 0, 1)
    grad_out = noise(seeds[5], (RESIDUES, RESIDUES, CHANNELS), 3.0, 18.0, ((0, 32), (1, 8)))
    return {"query_proj": query_proj, "key_proj": key_proj, "value_proj": value_proj, "pair_bias": pair_bias, "pair_mask": pair_mask, "grad_out": grad_out}


def block_grads(queries, keys_all, values_all, grads, mask_all, bias_full):
    block_rows, query_count, channel_count = queries.shape
    key_count = keys_all.shape[1]
    scale = 1.0 / math.sqrt(HEAD_DIM)
    query_heads = queries.astype(jnp.float32).reshape(block_rows, query_count, HEADS, HEAD_DIM)
    key_heads = keys_all.astype(jnp.float32).reshape(block_rows, key_count, HEADS, HEAD_DIM)
    value_heads = values_all.astype(jnp.float32).reshape(block_rows, key_count, HEADS, HEAD_DIM)
    grad_heads = grads.astype(jnp.float32).reshape(block_rows, query_count, HEADS, HEAD_DIM)
    masked = 1000000000.0 * (mask_all.astype(jnp.float32) - 1.0)
    scores = jnp.einsum('bjhd,bkhd->bhjk', query_heads, key_heads) * scale
    scores = scores + bias_full.astype(jnp.float32)[None] + masked[:, None, None, :]
    top_score = lax.optimization_barrier(jnp.max(scores, axis=-1, keepdims=True))
    weights = jnp.exp(scores - top_score)
    attn_probs = weights / lax.optimization_barrier(jnp.sum(weights, axis=-1, keepdims=True))
    attn_low = attn_probs.astype(jnp.bfloat16).astype(jnp.float32)
    attended = jnp.einsum('bhjk,bkhd->bjhd', attn_low, value_heads)
    row_delta = lax.optimization_barrier(jnp.sum(grad_heads * attended, axis=-1))
    grad_probs = jnp.einsum('bjhd,bkhd->bhjk', grad_heads, value_heads)
    grad_scores = attn_probs * (grad_probs - jnp.transpose(row_delta, (0, 2, 1))[..., None])
    scores_low = grad_scores.astype(jnp.bfloat16).astype(jnp.float32)
    grad_queries = jnp.einsum('bhjk,bkhd->bjhd', scores_low, key_heads) * scale
    grad_keys = jnp.einsum('bhjk,bjhd->bkhd', scores_low, query_heads) * scale
    grad_values = jnp.einsum('bhjk,bjhd->bkhd', attn_low, grad_heads)
    bias_grad = lax.optimization_barrier(jnp.sum(grad_scores, axis=0))
    return (grad_queries.reshape(block_rows, query_count, channel_count), grad_keys.reshape(block_rows, key_count, channel_count), grad_values.reshape(block_rows, key_count, channel_count), bias_grad)

def reference(query_proj, key_proj, value_proj, pair_bias, pair_mask, grad_out):
    block_rows = math.gcd(RESIDUES, 8)
    steps_count = RESIDUES // block_rows

    def split_rows(array):
        return array.reshape((steps_count, block_rows) + array.shape[1:])

    def one_block(bias_sum, pieces):
        grad_queries, grad_keys, grad_values, bias_grad = block_grads(pieces[0], pieces[1], pieces[2], pieces[3], pieces[4], pair_bias)
        return (bias_sum + bias_grad, (grad_queries.astype(jnp.bfloat16), grad_keys.astype(jnp.bfloat16), grad_values.astype(jnp.bfloat16)))
    start_sum = jnp.zeros((HEADS, RESIDUES, RESIDUES), jnp.float32)
    bias_sum, stacked = lax.scan(one_block, start_sum, (split_rows(query_proj), split_rows(key_proj), split_rows(value_proj), split_rows(grad_out), split_rows(pair_mask)))
    full_shape = (RESIDUES, RESIDUES, CHANNELS)
    return (stacked[0].reshape(full_shape), stacked[1].reshape(full_shape), stacked[2].reshape(full_shape), bias_sum)
```

```python
import math

import jax
import jax.numpy as jnp
from jax import lax
from jax.experimental import pallas as pl
from jax.experimental.pallas import tpu as pltpu
from jax.sharding import Mesh
from jax.sharding import PartitionSpec as P

HEADS = 4
HEAD_DIM = 32
LANES = 128
ROWS = ("zh", "x", "y")
COL = ("z", "core")
PLANE = ("x", "y")
COLUMN = ("zh", "z")
CHUNKS = 3
TILE = 256
BF16 = jnp.bfloat16
F32 = jnp.float32


def lane_slot(shape):
    return lax.broadcasted_iota(jnp.int32, shape, len(shape) - 1) // HEAD_DIM


def turned(value, slots):
    return pltpu.roll(value, (slots * HEAD_DIM) & (LANES - 1), value.ndim - 1)


def small_input():
    return pl.BlockSpec(memory_space=pltpu.SMEM)


def in_vmem(count):
    return [pl.BlockSpec(memory_space=pltpu.VMEM) for _ in range(count)]


def pack_body(place, *refs, with_mask):
    tensors = refs[:4]
    mask = refs[4] if with_mask else None
    outs = refs[-8:]
    z, core = place[0], place[1]
    rows, queries = tensors[0].shape[2], tensors[0].shape[3]
    slot = lane_slot((queries, LANES))

    def one_row(r, carry):
        for kc in range(2):
            half = core ^ kc
            parts = [t[half, 0, r].astype(F32) for t in tensors]
            for kz in range(4):
                head = z ^ kz
                packed = turned(parts[0], 4 - head)
                for t in range(1, 4):
                    packed = jnp.where(slot == t, turned(parts[t], 4 + t - head), packed)
                start = pl.multiple_of(r * queries, 16)
                outs[kz * 2 + kc][pl.ds(start, queries), :] = packed.astype(BF16)
        return carry

    lax.fori_loop(0, rows, one_row, 0)
    if with_mask:
        for k in range(8):
            outs[k][rows * queries :, :] = mask[core ^ (k & 1)]


def pack(place, tensors, mask, chunk):
    halves, chunks, rows, queries, _ = tensors[0].shape
    length = rows * queries + (0 if mask is None else 16)
    block = pl.BlockSpec((halves, 1, rows, queries, LANES), lambda i: (0, chunk, 0, 0, 0))
    operands = list(tensors)
    specs = [block] * 4
    if mask is not None:
        operands.append(mask)
        specs.append(pl.BlockSpec(mask.shape, lambda i: (0, 0, 0)))
    return pl.pallas_call(
        lambda *refs: pack_body(*refs, with_mask=mask is not None),
        grid=(1,),
        in_specs=[small_input()] + specs,
        out_specs=[pl.BlockSpec((length, LANES), lambda i: (0, 0))] * 8,
        out_shape=[jax.ShapeDtypeStruct((length, LANES), BF16)] * 8,
        cost_estimate=pl.CostEstimate(flops=10**9, bytes_accessed=2 * 10**6, transcendentals=0),
        name=f"pack{chunk}",
    )(place, *operands)


def position(place, k):
    return (k & 1) * 4 + (place[0] ^ (k >> 1))


def attention_body(place, *refs, first, rows):
    tiles = refs[:8]
    bias = refs[8]
    if first:
        (outs, bias_grad, mask_out), scratch = (refs[9:17], refs[17], refs[18]), refs[19:]
        mask_lanes = mask_out
    else:
        mask_lanes, bias_grad_in = refs[9], refs[10]
        (outs, bias_grad), scratch = (refs[11:19], refs[19]), refs[20:]
    pairs, probs, scores_low, logits, grad_probs, key_sum, value_sum, query_sum, masked = scratch
    length = pairs.shape[0]
    block = length // 8
    strip = block
    scale = 1.0 / math.sqrt(HEAD_DIM)

    if first:
        bias_grad[...] = jnp.zeros_like(bias_grad)
        pick = (
            lax.broadcasted_iota(jnp.int32, (16, LANES), 0)
            == lax.broadcasted_iota(jnp.int32, (16, LANES), 1)
        ).astype(BF16)
        for k in range(8):
            start = pl.multiple_of(position(place, k) * block, 16)
            columns = lax.dot_general(
                tiles[k][rows * block :, :], pick, (((0,), (0,)), ((), ())), preferred_element_type=F32
            )
            mask_out[pl.ds(start, block), :] = columns[:block].astype(BF16)
    else:
        bias_grad[...] = bias_grad_in[...]
    key_sum[...] = jnp.zeros_like(key_sum)
    value_sum[...] = jnp.zeros_like(value_sum)
    row_base = 0 if first else place[2]

    def one_row(r, carry):
        for k in range(8):
            start = pl.multiple_of(position(place, k) * block, 16)
            source = pl.multiple_of(r * block, 16)
            pairs[pl.ds(start, block), :] = tiles[k][pl.ds(source, block), :]
        slot = lane_slot((length, LANES))
        wide = pairs[...].astype(F32)
        zero = jnp.zeros_like(wide)
        query_at_key = jnp.where(slot == 1, pltpu.roll(wide, HEAD_DIM, 1), zero).astype(BF16)
        grad_at_value = jnp.where(slot == 2, pltpu.roll(wide, LANES - HEAD_DIM, 1), zero).astype(BF16)
        query_at_row = jnp.where(slot == r, turned(wide, r), zero).astype(BF16)
        grad_at_row = jnp.where(slot == r, turned(wide, r + 1), zero).astype(BF16)
        keys_turned = jnp.transpose(wide)[HEAD_DIM : 2 * HEAD_DIM, :].astype(BF16)
        chosen = (lax.broadcasted_iota(jnp.int32, (LANES, LANES), 0) == r + row_base).astype(BF16)
        masked[...] = 1000000000.0 * (
            jnp.dot(mask_lanes[...], chosen, preferred_element_type=F32) - 1.0
        )
        for j in range(0, length, TILE):
            right_query = query_at_key[j : j + TILE]
            right_grad = grad_at_value[j : j + TILE]
            top = jnp.full((8, TILE), -jnp.inf, F32)
            for i in range(0, length, strip):
                s = lax.dot_general(
                    pairs[i : i + strip, :],
                    right_query,
                    (((1,), (1,)), ((), ())),
                    preferred_element_type=F32,
                )
                mask_strip = masked[i : i + strip, :]
                t = (
                    s * scale
                    + bias[i : i + strip, j : j + TILE]
                    + jnp.concatenate([mask_strip] * (TILE // LANES), axis=1)
                )
                logits[i : i + strip, :] = t
                top = jnp.maximum(top, jnp.max(t.reshape(strip // 8, 8, TILE), axis=0))
            top = jnp.max(top, axis=0, keepdims=True)
            total = jnp.zeros((8, TILE), F32)
            delta = jnp.zeros((8, TILE), F32)
            for i in range(0, length, strip):
                gp = lax.dot_general(
                    pairs[i : i + strip, :],
                    right_grad,
                    (((1,), (1,)), ((), ())),
                    preferred_element_type=F32,
                )
                e = jnp.exp(logits[i : i + strip, :] - top)
                logits[i : i + strip, :] = e
                grad_probs[i : i + strip, :] = gp
                total = total + jnp.sum(e.reshape(strip // 8, 8, TILE), axis=0)
                delta = delta + jnp.sum((e * gp).reshape(strip // 8, 8, TILE), axis=0)
            inverse = 1.0 / jnp.sum(total, axis=0, keepdims=True)
            delta = jnp.sum(delta, axis=0, keepdims=True) * inverse
            for i in range(0, length, strip):
                p = logits[i : i + strip, :] * inverse
                ds = p * (grad_probs[i : i + strip, :] - delta)
                probs[i : i + strip, j : j + TILE] = p.astype(BF16)
                scores_low[i : i + strip, j : j + TILE] = ds.astype(BF16)
                bias_grad[i : i + strip, j : j + TILE] += ds
        value_sum[...] += jnp.dot(probs[...], grad_at_row, preferred_element_type=F32)
        key_sum[...] += jnp.dot(scores_low[...], query_at_row, preferred_element_type=F32)
        query_sum[pl.ds(pl.multiple_of(r * HEAD_DIM, 32), HEAD_DIM), :] = jnp.dot(
            keys_turned, scores_low[...], preferred_element_type=F32
        )
        return carry

    lax.fori_loop(0, rows, one_row, 0)
    probs[:, :LANES] = (jnp.transpose(query_sum[...]) * scale).astype(BF16)
    scores_low[:, :LANES] = (key_sum[...] * scale).astype(BF16)
    scores_low[:, LANES : 2 * LANES] = value_sum[...].astype(BF16)
    for k in range(8):
        start = pl.multiple_of(position(place, k) * block, 16)
        outs[k][:block, :] = probs[pl.ds(start, block), :LANES]
        outs[k][block : 2 * block, :] = scores_low[pl.ds(start, block), :LANES]
        outs[k][2 * block :, :] = scores_low[pl.ds(start, block), LANES : 2 * LANES]


def attention(place, tiles, bias, mask_lanes, bias_grad, chunk, rows):
    first = chunk == 0
    length = bias.shape[0]
    block = length // 8
    place = jnp.concatenate([place, jnp.full((1,), chunk * rows, jnp.int32)])
    operands = [*tiles, bias]
    if not first:
        operands += [mask_lanes, bias_grad]
    out_shape = [jax.ShapeDtypeStruct((3 * block, LANES), BF16)] * 8
    out_shape.append(jax.ShapeDtypeStruct((length, length), F32))
    if first:
        out_shape.append(jax.ShapeDtypeStruct((length, LANES), BF16))
    results = pl.pallas_call(
        lambda *refs: attention_body(*refs, first=first, rows=rows),
        in_specs=[small_input()] + in_vmem(len(operands)),
        out_specs=in_vmem(len(out_shape)),
        out_shape=out_shape,
        scratch_shapes=[
            pltpu.VMEM((length, LANES), BF16),
            pltpu.VMEM((length, length), BF16),
            pltpu.VMEM((length, length), BF16),
            pltpu.VMEM((length, TILE), F32),
            pltpu.VMEM((length, TILE), F32),
            pltpu.VMEM((length, LANES), F32),
            pltpu.VMEM((length, LANES), F32),
            pltpu.VMEM((LANES, length), F32),
            pltpu.VMEM((length, LANES), F32),
        ],
        input_output_aliases={} if first else {len(operands): 8},
        cost_estimate=pl.CostEstimate(
            flops=10**10, bytes_accessed=6 * 10**6, transcendentals=length * length * rows
        ),
        compiler_params=pltpu.CompilerParams(vmem_limit_bytes=40 * 2**20),
        name=f"attention{chunk}",
    )(place, *operands)
    if first:
        return results[:8], results[8], results[9]
    return results[:8], results[8], mask_lanes


def unpack_body(place, *refs, first):
    parts = refs[:8]
    outs = refs[-3:]
    z, core = place[0], place[1]
    rows, queries = outs[0].shape[2], outs[0].shape[3]
    slot = lane_slot((queries, LANES))
    for kc in range(2):
        half = core ^ kc
        for t in range(3):
            heads = [parts[kz * 2 + kc][t * queries : (t + 1) * queries, :].astype(F32) for kz in range(4)]
            for r in range(rows):
                row = turned(heads[0], 4 + z - r)
                for kz in range(1, 4):
                    head = z ^ kz
                    row = jnp.where(slot == head, turned(heads[kz], 4 + head - r), row)
                outs[t][half, 0, r] = row.astype(BF16)


def unpack(place, parts, outs, chunk, shape):
    first = outs is None
    halves, chunks, rows, queries, lanes = shape
    block = pl.BlockSpec((halves, 1, rows, queries, lanes), lambda i: (0, chunk, 0, 0, 0))
    piece = pl.BlockSpec(parts[0].shape, lambda i: (0, 0))
    kept = [] if first else list(outs)
    return pl.pallas_call(
        lambda *refs: unpack_body(*refs, first=first),
        grid=(1,),
        in_specs=[small_input()] + [piece] * 8 + [pl.BlockSpec(memory_space=pl.ANY)] * len(kept),
        out_specs=[block] * 3,
        out_shape=[jax.ShapeDtypeStruct(shape, BF16)] * 3,
        input_output_aliases={} if first else {9: 0, 10: 1, 11: 2},
        name=f"unpack{chunk}",
    )(place, *parts, *kept)


def bias_rows(place, length):
    block = length // 8
    for zh in range(2):
        for x in range(4):
            tile = zh * 4 + x
            start = (((tile & 1) ^ place[1]) * 4 + (tile >> 1)) * block
            for y in range(4):
                part = block // 4
                yield x * 4 + y, zh * part, part, pl.multiple_of(start + y * part, 8)


def bias_in_body(place, own, other, out):
    length = out.shape[0]
    half = length // 2
    for row, line, part, start in bias_rows(place, length):
        out[pl.ds(start, part), :half] = own[row, line : line + part, :].astype(F32)
        out[pl.ds(start, part), half:] = other[row, line : line + part, :].astype(F32)


def bias_out_body(place, whole, own, other):
    length = whole.shape[0]
    half = length // 2
    for row, line, part, start in bias_rows(place, length):
        own[row, line : line + part, :] = whole[pl.ds(start, part), :half]
        other[row, line : line + part, :] = whole[pl.ds(start, part), half:].astype(BF16)


def swapped(value, k, axes):
    count = lax.axis_size(axes)
    return lax.ppermute(value, axes, [(i, i ^ k) for i in range(count)])


def exchanged(value, axes):
    return lax.all_to_all(value, axes, split_axis=0, concat_axis=0, tiled=True)


def gathered_bias(place, pair_bias):
    heads, queries, keys = pair_bias.shape
    turned_bias = jnp.transpose(pair_bias, (0, 2, 1))
    both = jnp.concatenate([turned_bias] * 2, axis=0)
    column = exchanged(both, COLUMN)
    lines = jnp.transpose(column.reshape(2, heads, keys, queries), (0, 2, 1, 3))
    lines = lines.reshape(2 * keys, heads * queries)
    own = exchanged(jnp.broadcast_to(lines, (16, *lines.shape)), PLANE)
    other = swapped(own, 1, "core")
    length = 8 * queries
    return pl.pallas_call(
        bias_in_body,
        in_specs=[small_input()] + in_vmem(2),
        out_specs=in_vmem(1)[0],
        out_shape=jax.ShapeDtypeStruct((length, length), F32),
        compiler_params=pltpu.CompilerParams(vmem_limit_bytes=16 * 2**20),
        name="bias_in",
    )(place, own, other)


def reduced_bias(place, bias_grad, heads):
    length = bias_grad.shape[0]
    queries = length // 8
    keys = length // 32
    shape = (16, 2 * keys, length // 2)
    own, other = pl.pallas_call(
        bias_out_body,
        in_specs=[small_input()] + in_vmem(1),
        out_specs=in_vmem(2),
        out_shape=[jax.ShapeDtypeStruct(shape, F32), jax.ShapeDtypeStruct(shape, BF16)],
        compiler_params=pltpu.CompilerParams(vmem_limit_bytes=16 * 2**20),
        name="bias_out",
    )(place, bias_grad)
    own = (own + swapped(other, 1, "core").astype(F32)).astype(BF16)
    lines = jnp.sum(exchanged(own, PLANE).astype(F32), axis=0).astype(BF16)
    lines = jnp.transpose(lines.reshape(2, keys, heads, queries), (0, 2, 1, 3))
    column = exchanged(lines.reshape(2 * heads, keys, queries), COLUMN)
    column = jnp.sum(column.astype(F32).reshape(2, heads, keys, queries), axis=0)
    return jnp.transpose(column, (0, 2, 1))


def local(query_proj, key_proj, value_proj, pair_bias, pair_mask, grad_out):
    row_count, queries, lanes = query_proj.shape
    rows = row_count // 2 // CHUNKS
    shape = (2, CHUNKS, rows, queries, lanes)
    place = jnp.stack([lax.axis_index("z"), lax.axis_index("core")]).astype(jnp.int32)
    mask = pair_mask.reshape(2, row_count // 2, queries).astype(BF16)
    mask = jnp.pad(mask, ((0, 0), (0, 16 - row_count // 2), (0, lanes - queries)))
    tensors = [t.reshape(shape) for t in (query_proj, key_proj, value_proj, grad_out)]
    bias = gathered_bias(place, pair_bias)
    arrived = []
    for chunk in range(CHUNKS):
        packed = pack(place, tensors, mask if chunk == 0 else None, chunk)
        arrived.append([packed[0]] + [swapped(packed[k], k, COL) for k in range(1, 8)])
    outs = mask_lanes = bias_grad = None
    returned = []
    for chunk in range(CHUNKS):
        grads, bias_grad, mask_lanes = attention(
            place, arrived[chunk], bias, mask_lanes, bias_grad, chunk, rows
        )
        returned.append([grads[0]] + [swapped(grads[k], k, COL) for k in range(1, 8)])
    grad_bias = reduced_bias(place, bias_grad, HEADS)
    for chunk in range(CHUNKS):
        outs = unpack(place, returned[chunk], outs, chunk, shape)
    grads = [o.reshape(query_proj.shape) for o in outs]
    return (*grads, grad_bias)


def solution(mesh):
    torus = Mesh(mesh.devices.reshape(2, 4, 4, 4, 2), ("zh", "x", "y", "z", "core"))
    placed = (
        P(ROWS, COL, None),
        P(ROWS, COL, None),
        P(ROWS, COL, None),
        P(None, COL, ROWS),
        P(ROWS, COL),
        P(ROWS, COL, None),
    )
    return jax.shard_map(
        local,
        mesh=torus,
        in_specs=placed,
        out_specs=(P(ROWS, COL, None), P(ROWS, COL, None), P(ROWS, COL, None), P(None, COL, ROWS)),
        check_vma=False,
    )
```

```python
import math

import jax
import jax.numpy as jnp
from jax import lax
from jax.experimental import pallas as pl
from jax.experimental.pallas import tpu as pltpu
from jax.sharding import Mesh
from jax.sharding import PartitionSpec as P


HEADS = 4
HEAD_DIM = 32
LANES = 128
ROWS = ("zh", "x", "y")
COL = ("z", "core")
PLANE = ("x", "y")
COLUMN = ("zh", "z")
CHUNKS = ((0, 8), (8, 4))
GROUP = 4
FAR_FIRST = (6, 7, 4, 5, 2, 3, 1)
TILE = 256
BF16 = jnp.bfloat16
F32 = jnp.float32


def lane_slot(shape):
    return lax.broadcasted_iota(jnp.int32, shape, len(shape) - 1) // HEAD_DIM


def turned(value, slots):
    return pltpu.roll(value, (slots * HEAD_DIM) & (LANES - 1), value.ndim - 1)


def small_input():
    return pl.BlockSpec(memory_space=pltpu.SMEM)


def in_vmem(count):
    return [pl.BlockSpec(memory_space=pltpu.VMEM) for _ in range(count)]


def pack_body(place, *refs, with_mask):
    tensors = refs[:4]
    mask = refs[4] if with_mask else None
    outs = refs[-8:]
    z, core = place[0], place[1]
    rows, queries = tensors[0].shape[1], tensors[0].shape[2]
    slot = lane_slot((queries, LANES))

    def one_row(r, carry):
        for kc in range(2):
            half = core ^ kc
            parts = [t[half, r].astype(F32) for t in tensors]
            for kz in range(4):
                head = z ^ kz
                packed = turned(parts[0], 4 - head)
                for t in range(1, 4):
                    packed = jnp.where(slot == t, turned(parts[t], 4 + t - head), packed)
                start = pl.multiple_of(r * queries, 16)
                outs[kz * 2 + kc][pl.ds(start, queries), :] = packed.astype(BF16)
        return carry

    lax.fori_loop(0, rows, one_row, 0)
    if with_mask:
        for kc in range(2):
            count = mask.shape[0] // 2
            present = jnp.where((core ^ kc) == 0, mask[:count, :], mask[count:, :]).astype(F32)
            present = jnp.concatenate([present, jnp.zeros((16 - count, queries), F32)], axis=0)
            for kz in range(4):
                outs[kz * 2 + kc][rows * queries :, :queries] = present.astype(BF16)
                outs[kz * 2 + kc][rows * queries :, queries:] = jnp.zeros((16, LANES - queries), BF16)


def pack(place, tensors, mask, chunk):
    halves, _, queries, _ = tensors[0].shape
    first_row, rows = CHUNKS[chunk]
    length = rows * queries + (0 if mask is None else 16)
    block = pl.BlockSpec((halves, rows, queries, LANES), lambda i: (0, first_row // rows, 0, 0))
    operands = list(tensors)
    specs = [block] * 4
    if mask is not None:
        operands.append(mask)
        specs.append(pl.BlockSpec(mask.shape, lambda i: (0, 0)))
    return pl.pallas_call(
        lambda *refs: pack_body(*refs, with_mask=mask is not None),
        grid=(1,),
        in_specs=[small_input()] + specs,
        out_specs=[pl.BlockSpec((length, LANES), lambda i: (0, 0))] * 8,
        out_shape=[jax.ShapeDtypeStruct((length, LANES), BF16)] * 8,
        cost_estimate=pl.CostEstimate(flops=10**9, bytes_accessed=2 * 10**6, transcendentals=0),
    )(place, *operands)


def position(place, k):
    return (k & 1) * 4 + (place[0] ^ (k >> 1))


def attention_body(place, *refs, first_row, rows):
    first = first_row == 0
    tiles = refs[:8]
    bias = refs[8]
    if first:
        (outs, bias_grad, mask_out), scratch = (refs[9:17], refs[17], refs[18]), refs[19:]
        mask_lanes = mask_out
    else:
        mask_lanes, bias_grad_in = refs[9], refs[10]
        (outs, bias_grad), scratch = (refs[11:19], refs[19]), refs[20:]
    pairs, probs, scores_low, logits, grad_probs, key_sum, value_sum, query_sum, masked = scratch
    length = pairs.shape[0]
    block = length // 8
    strip = block
    scale = 1.0 / math.sqrt(HEAD_DIM)

    if first:
        bias_grad[...] = jnp.zeros_like(bias_grad)
        pick = (
            lax.broadcasted_iota(jnp.int32, (16, LANES), 0)
            == lax.broadcasted_iota(jnp.int32, (16, LANES), 1)
        ).astype(BF16)
        for k in range(8):
            start = pl.multiple_of(position(place, k) * block, 16)
            columns = lax.dot_general(
                tiles[k][rows * block :, :], pick, (((0,), (0,)), ((), ())), preferred_element_type=F32
            )
            mask_out[pl.ds(start, block), :] = columns[:block].astype(BF16)
    else:
        bias_grad[...] = bias_grad_in[...]
    key_sum[...] = jnp.zeros_like(key_sum)
    value_sum[...] = jnp.zeros_like(value_sum)
    groups = rows // GROUP

    def one_row(r, carry):
        for k in range(8):
            start = pl.multiple_of(position(place, k) * block, 16)
            source = pl.multiple_of(r * block, 16)
            pairs[pl.ds(start, block), :] = tiles[k][pl.ds(source, block), :]
        slot = lane_slot((length, LANES))
        wide = pairs[...].astype(F32)
        zero = jnp.zeros_like(wide)
        query_at_key = jnp.where(slot == 1, pltpu.roll(wide, HEAD_DIM, 1), zero).astype(BF16)
        grad_at_value = jnp.where(slot == 2, pltpu.roll(wide, LANES - HEAD_DIM, 1), zero).astype(BF16)
        group, in_group = r // GROUP, r % GROUP
        query_at_row = jnp.where(slot == in_group, turned(wide, in_group), zero).astype(BF16)
        grad_at_row = jnp.where(slot == in_group, turned(wide, in_group + 1), zero).astype(BF16)
        keys_turned = jnp.transpose(wide)[HEAD_DIM : 2 * HEAD_DIM, :].astype(BF16)
        chosen = (lax.broadcasted_iota(jnp.int32, (LANES, LANES), 0) == r + first_row).astype(BF16)
        masked[...] = 1000000000.0 * (
            jnp.dot(mask_lanes[...], chosen, preferred_element_type=F32) - 1.0
        )
        for j in range(0, length, TILE):
            right_query = query_at_key[j : j + TILE]
            right_grad = grad_at_value[j : j + TILE]
            top = jnp.full((8, TILE), -jnp.inf, F32)
            for i in range(0, length, strip):
                s = lax.dot_general(
                    pairs[i : i + strip, :],
                    right_query,
                    (((1,), (1,)), ((), ())),
                    preferred_element_type=F32,
                )
                mask_strip = masked[i : i + strip, :]
                t = (
                    s * scale
                    + bias[i : i + strip, j : j + TILE]
                    + jnp.concatenate([mask_strip] * (TILE // LANES), axis=1)
                )
                logits[i : i + strip, :] = t
                top = jnp.maximum(top, jnp.max(t.reshape(strip // 8, 8, TILE), axis=0))
            top = jnp.max(top, axis=0, keepdims=True)
            total = jnp.zeros((8, TILE), F32)
            delta = jnp.zeros((8, TILE), F32)
            for i in range(0, length, strip):
                gp = lax.dot_general(
                    pairs[i : i + strip, :],
                    right_grad,
                    (((1,), (1,)), ((), ())),
                    preferred_element_type=F32,
                )
                e = jnp.exp(logits[i : i + strip, :] - top)
                logits[i : i + strip, :] = e
                grad_probs[i : i + strip, :] = gp
                total = total + jnp.sum(e.reshape(strip // 8, 8, TILE), axis=0)
                delta = delta + jnp.sum((e * gp).reshape(strip // 8, 8, TILE), axis=0)
            inverse = 1.0 / jnp.sum(total, axis=0, keepdims=True)
            delta = jnp.sum(delta, axis=0, keepdims=True) * inverse
            for i in range(0, length, strip):
                p = logits[i : i + strip, :] * inverse
                ds = p * (grad_probs[i : i + strip, :] - delta)
                probs[i : i + strip, j : j + TILE] = p.astype(BF16)
                scores_low[i : i + strip, j : j + TILE] = ds.astype(BF16)
                bias_grad[i : i + strip, j : j + TILE] += ds
        value_sum[group] += jnp.dot(probs[...], grad_at_row, preferred_element_type=F32)
        key_sum[group] += jnp.dot(scores_low[...], query_at_row, preferred_element_type=F32)
        query_sum[pl.ds(pl.multiple_of(r * HEAD_DIM, 32), HEAD_DIM), :] = jnp.dot(
            keys_turned, scores_low[...], preferred_element_type=F32
        )
        return carry

    lax.fori_loop(0, rows, one_row, 0)
    for g in range(groups):
        lanes = pl.ds(g * LANES, LANES)
        probs[:, lanes] = (jnp.transpose(query_sum[lanes, :]) * scale).astype(BF16)
        scores_low[:, lanes] = (key_sum[g] * scale).astype(BF16)
        scores_low[:, pl.ds((groups + g) * LANES, LANES)] = value_sum[g].astype(BF16)
    for k in range(8):
        start = pl.multiple_of(position(place, k) * block, 16)
        for g in range(3 * groups):
            held, lane = (probs, g) if g < groups else (scores_low, g - groups)
            outs[k][g * block : (g + 1) * block, :] = held[
                pl.ds(start, block), lane * LANES : (lane + 1) * LANES
            ]


def attention(place, tiles, bias, mask_lanes, bias_grad, chunk):
    first = chunk == 0
    first_row, rows = CHUNKS[chunk]
    groups = rows // GROUP
    length = bias.shape[0]
    block = length // 8
    operands = [*tiles, bias]
    if not first:
        operands += [mask_lanes, bias_grad]
    out_shape = [jax.ShapeDtypeStruct((3 * groups * block, LANES), BF16)] * 8
    out_shape.append(jax.ShapeDtypeStruct((length, length), F32))
    if first:
        out_shape.append(jax.ShapeDtypeStruct((length, LANES), BF16))
    results = pl.pallas_call(
        lambda *refs: attention_body(*refs, first_row=first_row, rows=rows),
        in_specs=[small_input()] + in_vmem(len(operands)),
        out_specs=in_vmem(len(out_shape)),
        out_shape=out_shape,
        scratch_shapes=[
            pltpu.VMEM((length, LANES), BF16),
            pltpu.VMEM((length, length), BF16),
            pltpu.VMEM((length, length), BF16),
            pltpu.VMEM((length, TILE), F32),
            pltpu.VMEM((length, TILE), F32),
            pltpu.VMEM((groups, length, LANES), F32),
            pltpu.VMEM((groups, length, LANES), F32),
            pltpu.VMEM((groups * LANES, length), F32),
            pltpu.VMEM((length, LANES), F32),
        ],
        input_output_aliases={} if first else {len(operands): 8},
        cost_estimate=pl.CostEstimate(
            flops=10**10, bytes_accessed=6 * 10**6, transcendentals=length * length * rows
        ),
        compiler_params=pltpu.CompilerParams(vmem_limit_bytes=40 * 2**20),
    )(place, *operands)
    if first:
        return results[:8], results[8], results[9]
    return results[:8], results[8], mask_lanes


def unpack_body(place, *refs):
    parts = refs[:8]
    outs = refs[-3:]
    z, core = place[0], place[1]
    rows, queries = outs[0].shape[1], outs[0].shape[2]
    groups = rows // GROUP
    slot = lane_slot((queries, LANES))
    for kc in range(2):
        half = core ^ kc
        for g in range(3 * groups):
            heads = [parts[kz * 2 + kc][g * queries : (g + 1) * queries, :].astype(F32) for kz in range(4)]
            for r in range(GROUP):
                row = turned(heads[0], 4 + z - r)
                for kz in range(1, 4):
                    head = z ^ kz
                    row = jnp.where(slot == head, turned(heads[kz], 4 + head - r), row)
                outs[g // groups][half, g % groups * GROUP + r] = row.astype(BF16)


def unpack(place, parts, outs, chunk, shape):
    first = outs is None
    halves, _, queries, lanes = shape
    first_row, rows = CHUNKS[chunk]
    block = pl.BlockSpec((halves, rows, queries, lanes), lambda i: (0, first_row // rows, 0, 0))
    piece = pl.BlockSpec(parts[0].shape, lambda i: (0, 0))
    kept = [] if first else list(outs)
    return pl.pallas_call(
        lambda *refs: unpack_body(*refs),
        grid=(1,),
        in_specs=[small_input()] + [piece] * 8 + [pl.BlockSpec(memory_space=pl.ANY)] * len(kept),
        out_specs=[block] * 3,
        out_shape=[jax.ShapeDtypeStruct(shape, BF16)] * 3,
        input_output_aliases={} if first else {9: 0, 10: 1, 11: 2},
    )(place, *parts, *kept)


def bias_rows(place, length):
    block = length // 8
    for zh in range(2):
        for x in range(4):
            tile = zh * 4 + x
            start = (((tile & 1) ^ place[1]) * 4 + (tile >> 1)) * block
            for y in range(4):
                part = block // 4
                yield x * 4 + y, zh * part, part, pl.multiple_of(start + y * part, 8)


def bias_in_body(place, own, other, out):
    length = out.shape[0]
    half = length // 2
    for row, line, part, start in bias_rows(place, length):
        out[pl.ds(start, part), :half] = own[row, line : line + part, :].astype(F32)
        out[pl.ds(start, part), half:] = other[row, line : line + part, :].astype(F32)


def bias_out_body(place, whole, own, other):
    length = whole.shape[0]
    half = length // 2
    for row, line, part, start in bias_rows(place, length):
        own[row, line : line + part, :] = whole[pl.ds(start, part), :half]
        other[row, line : line + part, :] = whole[pl.ds(start, part), half:].astype(BF16)


def swapped(value, k, axes):
    count = lax.axis_size(axes)
    return lax.ppermute(value, axes, [(i, i ^ k) for i in range(count)])


def sent(values):
    arrived = dict.fromkeys(range(8))
    arrived[0] = values[0]
    for k in FAR_FIRST:
        arrived[k] = swapped(values[k], k, COL)
    return list(arrived.values())


def exchanged(value, axes):
    return lax.all_to_all(value, axes, split_axis=0, concat_axis=0, tiled=True)


def gathered_bias(place, pair_bias):
    heads, queries, keys = pair_bias.shape
    turned_bias = jnp.transpose(pair_bias, (0, 2, 1))
    both = jnp.concatenate([turned_bias] * 2, axis=0)
    column = exchanged(both, COLUMN)
    lines = jnp.transpose(column.reshape(2, heads, keys, queries), (0, 2, 1, 3))
    lines = lines.reshape(2 * keys, heads * queries)
    own = exchanged(jnp.broadcast_to(lines, (16, *lines.shape)), PLANE)
    other = swapped(own, 1, "core")
    length = 8 * queries
    return pl.pallas_call(
        bias_in_body,
        in_specs=[small_input()] + in_vmem(2),
        out_specs=in_vmem(1)[0],
        out_shape=jax.ShapeDtypeStruct((length, length), F32),
        compiler_params=pltpu.CompilerParams(vmem_limit_bytes=16 * 2**20),
        name="bias_in",
    )(place, own, other)


def reduced_bias(place, bias_grad, heads):
    length = bias_grad.shape[0]
    queries = length // 8
    keys = length // 32
    shape = (16, 2 * keys, length // 2)
    own, other = pl.pallas_call(
        bias_out_body,
        in_specs=[small_input()] + in_vmem(1),
        out_specs=in_vmem(2),
        out_shape=[jax.ShapeDtypeStruct(shape, F32), jax.ShapeDtypeStruct(shape, BF16)],
        compiler_params=pltpu.CompilerParams(vmem_limit_bytes=16 * 2**20),
        name="bias_out",
    )(place, bias_grad)
    own = (own + swapped(other, 1, "core").astype(F32)).astype(BF16)
    lines = jnp.sum(exchanged(own, PLANE).astype(F32), axis=0).astype(BF16)
    lines = jnp.transpose(lines.reshape(2, keys, heads, queries), (0, 2, 1, 3))
    column = exchanged(lines.reshape(2 * heads, keys, queries), COLUMN)
    column = jnp.sum(column.astype(F32).reshape(2, heads, keys, queries), axis=0)
    return jnp.transpose(column, (0, 2, 1))


def all_rows(query_proj, key_proj, value_proj, pair_bias, pair_mask, grad_out):
    row_count, queries, lanes = query_proj.shape
    shape = (2, row_count // 2, queries, lanes)
    place = jnp.stack([lax.axis_index("z"), lax.axis_index("core")]).astype(jnp.int32)
    tensors = [t.reshape(shape) for t in (query_proj, key_proj, value_proj, grad_out)]
    bias = gathered_bias(place, pair_bias)
    chunks = range(len(CHUNKS))
    arrived = []
    for chunk in chunks:
        packed = pack(place, tensors, pair_mask if chunk == 0 else None, chunk)
        arrived.append(sent(packed))
    outs = mask_lanes = bias_grad = None
    returned = []
    for chunk in chunks:
        grads, bias_grad, mask_lanes = attention(place, arrived[chunk], bias, mask_lanes, bias_grad, chunk)
        returned.append(sent(grads))
    grad_bias = reduced_bias(place, bias_grad, HEADS)
    for chunk in chunks:
        outs = unpack(place, returned[chunk], outs, chunk, shape)
    grads = [o.reshape(query_proj.shape) for o in outs]
    return (*grads, grad_bias)


def solution(mesh):
    torus = Mesh(mesh.devices.reshape(2, 4, 4, 4, 2), ("zh", "x", "y", "z", "core"))
    placed = (
        P(ROWS, COL, None),
        P(ROWS, COL, None),
        P(ROWS, COL, None),
        P(None, COL, ROWS),
        P(ROWS, COL),
        P(ROWS, COL, None),
    )
    return jax.shard_map(
        all_rows,
        mesh=torus,
        in_specs=placed,
        out_specs=(P(ROWS, COL, None), P(ROWS, COL, None), P(ROWS, COL, None), P(None, COL, ROWS)),
        check_vma=False,
    )
```

```python
import math

import jax
import jax.numpy as jnp
from jax import lax
from jax.experimental import pallas as pl
from jax.experimental.pallas import tpu as pltpu
from jax.sharding import Mesh
from jax.sharding import PartitionSpec as P


HEADS = 4
HEAD_DIM = 32
LANES = 128
ROWS = ("zh", "x", "y")
COL = ("z", "core")
PLANE = ("x", "y")
COLUMN = ("zh", "z")
CHUNKS = ((0, 4), (4, 4), (8, 4))
SENDS = ((0, 8), (8, 4))
GROUP = 4
STRIP = 768
FAR_FIRST = (6, 7, 4, 5, 2, 3, 1)
TILE = 256
BF16 = jnp.bfloat16
F32 = jnp.float32

LOG2E = math.log2(math.e)


def lane_slot(shape):
    return lax.broadcasted_iota(jnp.int32, shape, len(shape) - 1) // HEAD_DIM


def turned(value, slots):
    shift = slots * HEAD_DIM & (LANES - 1)
    return value if isinstance(shift, int) and shift == 0 else pltpu.roll(value, shift, value.ndim - 1)


def small_input():
    return pl.BlockSpec(memory_space=pltpu.SMEM)


def in_vmem(count):
    return [pl.BlockSpec(memory_space=pltpu.VMEM) for _ in range(count)]


def pack_body(place, *refs, with_mask):
    tensors = refs[:4]
    mask = refs[4] if with_mask else None
    outs, held = refs[-9:-1], refs[-1]
    z, core = place[0], place[1]
    rows, queries = tensors[0].shape[1], tensors[0].shape[2]
    slot = lane_slot((queries, LANES))

    def one_row(r, carry):
        for kc in range(2):
            half = core ^ kc
            parts = [t[half, r] for t in tensors]
            for head in range(HEADS):
                packed = turned(parts[0], -head)
                for t in range(1, 4):
                    packed = jnp.where(slot == t, turned(parts[t], t - head), packed)
                held[head] = packed
            start = pl.multiple_of(r * queries, 16)
            for kz in range(4):
                outs[kz * 2 + kc][pl.ds(start, queries), :] = held[z ^ kz]
        return carry

    lax.fori_loop(0, rows, one_row, 0)
    if with_mask:
        for kc in range(2):
            count = mask.shape[0] // 2
            present = jnp.where((core ^ kc) == 0, mask[:count, :], mask[count:, :]).astype(F32)
            present = jnp.concatenate([present, jnp.zeros((16 - count, queries), F32)], axis=0)
            for kz in range(4):
                outs[kz * 2 + kc][rows * queries :, :queries] = present.astype(BF16)
                outs[kz * 2 + kc][rows * queries :, queries:] = jnp.zeros((16, LANES - queries), BF16)


def pack(place, tensors, mask, chunk):
    halves, _, queries, _ = tensors[0].shape
    first_row, rows = CHUNKS[chunk]
    length = rows * queries + (0 if mask is None else 16)
    block = pl.BlockSpec((halves, rows, queries, LANES), lambda i: (0, first_row // rows, 0, 0))
    operands = list(tensors)
    specs = [block] * 4
    if mask is not None:
        operands.append(mask)
        specs.append(pl.BlockSpec(mask.shape, lambda i: (0, 0)))
    return pl.pallas_call(
        lambda *refs: pack_body(*refs, with_mask=mask is not None),
        grid=(1,),
        in_specs=[small_input()] + specs,
        out_specs=[pl.BlockSpec((length, LANES), lambda i: (0, 0))] * 8,
        out_shape=[jax.ShapeDtypeStruct((length, LANES), BF16)] * 8,
        scratch_shapes=[pltpu.VMEM((HEADS, queries, LANES), BF16)],
        cost_estimate=pl.CostEstimate(flops=10**9, bytes_accessed=2 * 10**6, transcendentals=0),
    )(place, *operands)


def position(place, k):
    return (k & 1) * 4 + (place[0] ^ (k >> 1))


def attention_body(place, *refs, first, first_row, rows, held_count):
    tiles, refs = refs[:8], refs[8:]
    held, refs = refs[:held_count], refs[held_count:]
    bias, refs = refs[0], refs[1:]
    if not first:
        mask_lanes, bias_grad_in, refs = refs[0], refs[1], refs[2:]
    outs, bias_grad, refs = refs[:8], refs[8], refs[9:]
    if first:
        mask_lanes, refs = refs[0], refs[1:]
        mask_out = mask_lanes
    scratch = refs
    held_groups = 0 if not held else held[0].shape[0] // (3 * (bias.shape[0] // 8))
    pairs, left_key, left_value, masked, probs, scores_low, l0, l1, l2, g0, g1, g2, key_sum, value_sum, query_sum = scratch
    logits_all, grad_probs_all = (l0, l1, l2), (g0, g1, g2)
    zero_row = place[2]
    length = pairs.shape[0]
    block = length // 8
    scale = 1.0 / math.sqrt(HEAD_DIM)

    if first:
        bias_grad[...] = jnp.zeros_like(bias_grad)
        pick = (
            lax.broadcasted_iota(jnp.int32, (16, LANES), 0)
            == lax.broadcasted_iota(jnp.int32, (16, LANES), 1)
        ).astype(BF16)
        for k in range(8):
            start = pl.multiple_of(position(place, k) * block, 16)
            columns = lax.dot_general(
                tiles[k][rows * block :, :], pick, (((0,), (0,)), ((), ())), preferred_element_type=F32
            )
            mask_out[pl.ds(start, block), :] = columns[:block].astype(BF16)
    else:
        bias_grad[...] = bias_grad_in[...]
    key_sum[...] = jnp.zeros_like(key_sum)
    value_sum[...] = jnp.zeros_like(value_sum)
    groups = rows // GROUP

    def one_row(r, carry):
        for k in range(8):
            source = pl.ds(pl.multiple_of(r * block, 16), block)
            start = pl.multiple_of(position(place, k) * block, 16)
            pairs[pl.ds(start, block), :] = tiles[k][source, :]
        group, in_group = r // GROUP, r % GROUP
        slot = lane_slot((block, LANES))
        chosen = (lax.broadcasted_iota(jnp.int32, (LANES, LANES), 0) == r + first_row).astype(BF16)
        for i in range(0, length, block):
            own = slice(i, i + block)
            wide = pltpu.roll(pairs[own, :].astype(F32), LANES - HEAD_DIM, 1)
            left_key[own, :] = jnp.where(slot == 0, wide, 0.0).astype(BF16)
            wide = pltpu.roll(wide, 2 * HEAD_DIM, 1)
            left_value[own, :] = jnp.where(slot == 3, wide, 0.0).astype(BF16)
            present = jnp.dot(mask_lanes[own, :], chosen, preferred_element_type=F32)
            masked[own, :] = (1000000000.0 * LOG2E) * (present - 1.0)
        keys_turned = jnp.transpose(pairs[...].astype(F32))[HEAD_DIM : 2 * HEAD_DIM, :].astype(BF16)
        for tile, j in enumerate(range(0, length, TILE)):
            logits, grad_probs = logits_all[tile], grad_probs_all[tile]
            right = pairs[j : j + TILE, :]
            top = jnp.full((8, TILE), -jnp.inf, F32)
            for i in range(0, length, STRIP):
                t = lax.dot_general(
                    left_key[i : i + STRIP, :],
                    right,
                    (((1,), (1,)), ((), ())),
                    preferred_element_type=F32,
                )
                mask_strip = masked[i : i + STRIP, :]
                t = (
                    t * (scale * LOG2E)
                    + bias[i : i + STRIP, j : j + TILE]
                    + jnp.concatenate([mask_strip] * (TILE // LANES), axis=1)
                )
                logits[i : i + STRIP, :] = t
                top = jnp.maximum(top, jnp.max(t.reshape(STRIP // 8, 8, TILE), axis=0))
            for i in range(0, length, STRIP):
                grad_probs[i : i + STRIP, :] = lax.dot_general(
                    left_value[i : i + STRIP, :],
                    right,
                    (((1,), (1,)), ((), ())),
                    preferred_element_type=F32,
                )
            top = jnp.max(top, axis=0, keepdims=True)
            total = jnp.zeros((8, TILE), F32)
            delta = jnp.zeros((8, TILE), F32)
            for i in range(0, length, 32):
                held = pl.ds(pl.multiple_of(zero_row + i, 8), 32)
                gp = grad_probs[i : i + 32, :]
                e = jnp.exp2(logits[i : i + 32, :] - top)
                logits[i : i + 32, :] = e
                total = total + jnp.sum(e.reshape(4, 8, TILE), axis=0)
                delta = delta + jnp.sum((e * gp).reshape(4, 8, TILE), axis=0)
            inverse = 1.0 / jnp.sum(total, axis=0, keepdims=True)
            delta = jnp.sum(delta, axis=0, keepdims=True) * inverse
            for i in range(0, length, 32):
                held = pl.ds(pl.multiple_of(zero_row + i, 8), 32)
                p = logits[held, :] * inverse
                ds = p * (grad_probs[held, :] - delta)
                probs[i : i + 32, j : j + TILE] = p.astype(BF16)
                scores_low[i : i + 32, j : j + TILE] = ds.astype(BF16)
                bias_grad[i : i + 32, j : j + TILE] += ds
        slot = lane_slot((length, LANES))
        value_row = jnp.dot(probs[...], pairs[...], preferred_element_type=F32)
        value_sum[group] = jnp.where(slot == in_group, turned(value_row, in_group + 1), value_sum[group])
        key_row = jnp.dot(scores_low[...], pairs[...], preferred_element_type=F32)
        key_sum[group] = jnp.where(slot == in_group, turned(key_row, in_group), key_sum[group])
        query_sum[pl.ds(pl.multiple_of(r * HEAD_DIM, 32), HEAD_DIM), :] = jnp.dot(
            keys_turned, scores_low[...], preferred_element_type=F32
        )
        return carry

    lax.fori_loop(0, rows, one_row, 0)
    for g in range(groups):
        lanes = pl.ds(g * LANES, LANES)
        probs[:, lanes] = (jnp.transpose(query_sum[lanes, :]) * scale).astype(BF16)
        scores_low[:, lanes] = (key_sum[g] * scale).astype(BF16)
        scores_low[:, pl.ds((groups + g) * LANES, LANES)] = value_sum[g].astype(BF16)
    for k in range(8):
        start = pl.multiple_of(position(place, k) * block, 16)
        for t in range(3):
            for g in range(held_groups + groups):
                line = (t * (held_groups + groups) + g) * block
                if g < held_groups:
                    own = (t * held_groups + g) * block
                    outs[k][line : line + block, :] = held[k][own : own + block, :]
                    continue
                source, lane = (probs, 0) if t == 0 else (scores_low, (t - 1) * groups)
                lane = (lane + g - held_groups) * LANES
                outs[k][line : line + block, :] = source[pl.ds(start, block), lane : lane + LANES]


def attention(place, tiles, held, bias, mask_lanes, bias_grad, chunk):
    first = chunk == 0
    first_row, rows = CHUNKS[chunk]
    groups = rows // GROUP
    length = bias.shape[0]
    block = length // 8
    place = jnp.concatenate([place, jnp.zeros((1,), jnp.int32)])
    operands = [*tiles, *held, bias]
    if not first:
        operands += [mask_lanes, bias_grad]
    lines = 3 * groups * block + (held[0].shape[0] if held else 0)
    out_shape = [jax.ShapeDtypeStruct((lines, LANES), BF16)] * 8
    out_shape.append(jax.ShapeDtypeStruct((length, length), F32))
    if first:
        out_shape.append(jax.ShapeDtypeStruct((length, LANES), BF16))
    results = pl.pallas_call(
        lambda *refs: attention_body(
            *refs, first=first, first_row=first_row, rows=rows, held_count=len(held)
        ),
        in_specs=[small_input()] + in_vmem(len(operands)),
        out_specs=in_vmem(len(out_shape)),
        out_shape=out_shape,
        scratch_shapes=[
            *[pltpu.VMEM((length, LANES), BF16)] * 3,
            pltpu.VMEM((length, LANES), F32),
            pltpu.VMEM((length, length), BF16),
            pltpu.VMEM((length, length), BF16),
            *[pltpu.VMEM((length, TILE), F32)] * 6,
            pltpu.VMEM((groups, length, LANES), F32),
            pltpu.VMEM((groups, length, LANES), F32),
            pltpu.VMEM((groups * LANES, length), F32),
        ],
        input_output_aliases={} if first else {len(operands): 8},
        cost_estimate=pl.CostEstimate(
            flops=10**10, bytes_accessed=6 * 10**6, transcendentals=length * length * rows
        ),
        compiler_params=pltpu.CompilerParams(vmem_limit_bytes=18 * 2**20),
    )(place, *operands)
    if first:
        return results[:8], results[8], results[9]
    return results[:8], results[8], mask_lanes


def unpack_body(place, *refs):
    parts = refs[:8]
    outs, held = refs[-4:-1], refs[-1]
    z, core = place[0], place[1]
    rows, queries = outs[0].shape[1], outs[0].shape[2]
    groups = rows // GROUP
    slot = lane_slot((queries, LANES))
    for kc in range(2):
        half = core ^ kc
        for g in range(3 * groups):
            for kz in range(4):
                held[z ^ kz] = parts[kz * 2 + kc][g * queries : (g + 1) * queries, :]
            heads = [held[h] for h in range(HEADS)]
            for r in range(GROUP):
                row = turned(heads[0], -r)
                for h in range(1, HEADS):
                    row = jnp.where(slot == h, turned(heads[h], h - r), row)
                outs[g // groups][half, g % groups * GROUP + r] = row


def unpack(place, parts, outs, chunk, shape):
    first = outs is None
    halves, _, queries, lanes = shape
    first_row, rows = SENDS[chunk]
    block = pl.BlockSpec((halves, rows, queries, lanes), lambda i: (0, first_row // rows, 0, 0))
    piece = pl.BlockSpec(parts[0].shape, lambda i: (0, 0))
    kept = [] if first else list(outs)
    return pl.pallas_call(
        lambda *refs: unpack_body(*refs),
        grid=(1,),
        in_specs=[small_input()] + [piece] * 8 + [pl.BlockSpec(memory_space=pl.ANY)] * len(kept),
        out_specs=[block] * 3,
        out_shape=[jax.ShapeDtypeStruct(shape, BF16)] * 3,
        scratch_shapes=[pltpu.VMEM((HEADS, queries, lanes), BF16)],
        input_output_aliases={} if first else {9: 0, 10: 1, 11: 2},
    )(place, *parts, *kept)


def bias_rows(place, length):
    block = length // 8
    for zh in range(2):
        for x in range(4):
            tile = zh * 4 + x
            start = (((tile & 1) ^ place[1]) * 4 + (tile >> 1)) * block
            for y in range(4):
                part = block // 4
                yield x * 4 + y, zh * part, part, pl.multiple_of(start + y * part, 8)


def bias_in_body(place, own, other, out):
    length = out.shape[0]
    half = length // 2
    for row, line, part, start in bias_rows(place, length):
        out[pl.ds(start, part), :half] = own[row, line : line + part, :].astype(F32) * LOG2E
        out[pl.ds(start, part), half:] = other[row, line : line + part, :].astype(F32) * LOG2E


def bias_out_body(place, whole, own, other):
    length = whole.shape[0]
    half = length // 2
    for row, line, part, start in bias_rows(place, length):
        own[row, line : line + part, :] = whole[pl.ds(start, part), :half]
        other[row, line : line + part, :] = whole[pl.ds(start, part), half:].astype(BF16)


def swapped(value, k, axes):
    count = lax.axis_size(axes)
    return lax.ppermute(value, axes, [(i, i ^ k) for i in range(count)])


def sent(values):
    arrived = dict.fromkeys(range(8))
    arrived[0] = values[0]
    for k in FAR_FIRST:
        arrived[k] = swapped(values[k], k, COL)
    return list(arrived.values())


def exchanged(value, axes):
    return lax.all_to_all(value, axes, split_axis=0, concat_axis=0, tiled=True)


def gathered_bias(place, pair_bias):
    heads, queries, keys = pair_bias.shape
    turned_bias = jnp.transpose(pair_bias, (0, 2, 1))
    both = jnp.concatenate([turned_bias] * 2, axis=0)
    column = exchanged(both, COLUMN)
    lines = jnp.transpose(column.reshape(2, heads, keys, queries), (0, 2, 1, 3))
    lines = lines.reshape(2 * keys, heads * queries)
    own = exchanged(jnp.broadcast_to(lines, (16, *lines.shape)), PLANE)
    other = swapped(own, 1, "core")
    length = 8 * queries
    return pl.pallas_call(
        bias_in_body,
        in_specs=[small_input()] + in_vmem(2),
        out_specs=in_vmem(1)[0],
        out_shape=jax.ShapeDtypeStruct((length, length), F32),
        compiler_params=pltpu.CompilerParams(vmem_limit_bytes=16 * 2**20),
        name="bias_in",
    )(place, own, other)


def reduced_bias(place, bias_grad, heads):
    length = bias_grad.shape[0]
    queries = length // 8
    keys = length // 32
    shape = (16, 2 * keys, length // 2)
    own, other = pl.pallas_call(
        bias_out_body,
        in_specs=[small_input()] + in_vmem(1),
        out_specs=in_vmem(2),
        out_shape=[jax.ShapeDtypeStruct(shape, F32), jax.ShapeDtypeStruct(shape, BF16)],
        compiler_params=pltpu.CompilerParams(vmem_limit_bytes=16 * 2**20),
        name="bias_out",
    )(place, bias_grad)
    own = (own + swapped(other, 1, "core").astype(F32)).astype(BF16)
    lines = jnp.sum(exchanged(own, PLANE).astype(F32), axis=0).astype(BF16)
    lines = jnp.transpose(lines.reshape(2, keys, heads, queries), (0, 2, 1, 3))
    column = exchanged(lines.reshape(2 * heads, keys, queries), COLUMN)
    column = jnp.sum(column.astype(F32).reshape(2, heads, keys, queries), axis=0)
    return jnp.transpose(column, (0, 2, 1))


def all_rows(query_proj, key_proj, value_proj, pair_bias, pair_mask, grad_out):
    row_count, queries, lanes = query_proj.shape
    shape = (2, row_count // 2, queries, lanes)
    place = jnp.stack([lax.axis_index("z"), lax.axis_index("core")]).astype(jnp.int32)
    tensors = [t.reshape(shape) for t in (query_proj, key_proj, value_proj, grad_out)]
    bias = gathered_bias(place, pair_bias)
    arrived = []
    for chunk in range(len(CHUNKS)):
        packed = pack(place, tensors, pair_mask if chunk == 0 else None, chunk)
        arrived.append(sent(packed))
    grads, bias_grad, mask_lanes = attention(place, arrived[0], [], bias, None, None, 0)
    grads, bias_grad, mask_lanes = attention(place, arrived[1], grads, bias, mask_lanes, bias_grad, 1)
    returned = [sent(grads)]
    grads, bias_grad, mask_lanes = attention(place, arrived[2], [], bias, mask_lanes, bias_grad, 2)
    returned.append(sent(grads))
    grad_bias = reduced_bias(place, bias_grad, HEADS)
    outs = None
    for chunk in range(len(SENDS)):
        outs = unpack(place, returned[chunk], outs, chunk, shape)
    grads = [o.reshape(query_proj.shape) for o in outs]
    return (*grads, grad_bias)


def solution(mesh):
    torus = Mesh(mesh.devices.reshape(2, 4, 4, 4, 2), ("zh", "x", "y", "z", "core"))
    placed = (
        P(ROWS, COL, None),
        P(ROWS, COL, None),
        P(ROWS, COL, None),
        P(None, COL, ROWS),
        P(ROWS, COL),
        P(ROWS, COL, None),
    )
    return jax.shard_map(
        all_rows,
        mesh=torus,
        in_specs=placed,
        out_specs=(P(ROWS, COL, None), P(ROWS, COL, None), P(ROWS, COL, None), P(None, COL, ROWS)),
        check_vma=False,
    )
```
